128 devices in a mesh: dp: 1, ep: 128 (over z, y, x, core).
Axes of the slice: x: 4, y: 4, z: 4, core: 2. Of those that a mesh axis runs over, the one named last changes fastest.
Arguments:
- hidden: bfloat16 [2, 128, 64, 2048], P(None, ('dp', 'ep'))
- expert_ids: int32 [2, 128, 64, 8], P(None, ('dp', 'ep'))
- gate_wts: float32 [2, 128, 64, 8], P(None, ('dp', 'ep'))
- w_query: bfloat16 [2048, 32, 128], replicated
- w_key: bfloat16 [2048, 32, 128], replicated
- w_value: bfloat16 [2048, 32, 128], replicated
- w_out: bfloat16 [32, 128, 2048], replicated
- attn_gain: bfloat16 [2048], replicated
- moe_gain: bfloat16 [2048], replicated
- w_gate: bfloat16 [128, 2048, 768], P('ep')
- w_up: bfloat16 [128, 2048, 768], P('ep')
- w_down: bfloat16 [128, 768, 2048], P('ep')
Outputs:
- output: bfloat16 [2, 128, 64, 2048], P(None, ('dp', 'ep'))
All inputs are finite; a program needn't handle non-finite values.
Results may differ from the reference program's by a relative error of at most 0.0105002.
Values are sent between devices in bfloat16 or wider.
A program may use at most 1 GiB of HBM per device.

```python
import jax
import jax.numpy as jnp
import numpy as np
from jax import lax

D_MODEL = 2048
N_HEADS = 32
HEAD_DIM = 128
FF_DIM = 768
N_EXPERTS = 128
TOP_K = 8
TOK_DEV = 64
SEQ_LEN = 64
GROUP_SIZE = 128

TOKENS = GROUP_SIZE * TOK_DEV
SEQ_COUNT = TOKENS // SEQ_LEN
PROJ_COLS = N_HEADS * HEAD_DIM
LOCAL_EXPERTS = N_EXPERTS // GROUP_SIZE
MEAN_ROWS = TOP_K * TOK_DEV // GROUP_SIZE
EXPERT_CAP = (3 * TOP_K * TOK_DEV + N_EXPERTS - 1) // N_EXPERTS
EXPERT_WINDOW = GROUP_SIZE * EXPERT_CAP
NORM_EPS = 1e-6


def dest_tables(hot_rows):
    rest_rows = GROUP_SIZE * MEAN_ROWS - hot_rows
    base_rows = rest_rows // (GROUP_SIZE - 1)
    extra_rows = rest_rows % (GROUP_SIZE - 1)
    row_counts = np.array([hot_rows] + [base_rows + 1] * extra_rows + [base_rows] * (GROUP_SIZE - 1 - extra_rows))
    dest_label = np.repeat(np.arange(GROUP_SIZE), row_counts)
    first_pos = np.repeat(np.cumsum(row_counts) - row_counts, row_counts)
    local_label = (np.arange(TOP_K * TOK_DEV) - first_pos) % LOCAL_EXPERTS
    return dest_label, local_label


def draw_routing(rng_key, hot_rows):
    dest_label, local_label = dest_tables(hot_rows)
    pair_count = TOP_K * TOK_DEV
    key_rot, key_perm, key_off = jax.random.split(rng_key, 3)
    rotation = jax.random.randint(key_rot, (), 0, GROUP_SIZE)
    pair_order = jax.random.permutation(key_perm, jnp.broadcast_to(jnp.arange(pair_count), (GROUP_SIZE, pair_count)), axis=1, independent=True)
    offsets = jax.random.randint(key_off, (GROUP_SIZE, GROUP_SIZE), 0, LOCAL_EXPERTS)
    dest_rel = jnp.asarray(dest_label)[pair_order]
    local_rel = jnp.asarray(local_label)[pair_order]
    local_ids = (local_rel + jnp.take_along_axis(offsets, dest_rel, axis=1)) % LOCAL_EXPERTS
    dest_ids = (dest_rel + rotation) % GROUP_SIZE
    expert_ids = (dest_ids * LOCAL_EXPERTS + local_ids).astype(jnp.int32)
    return expert_ids.reshape(SEQ_COUNT, SEQ_LEN, TOP_K)


def setup_inputs(seed: int = 0, part: int = 0) -> dict:
    shared_keys = jax.random.split(jax.random.key(seed), 9)
    part_keys = jax.random.split(jax.random.fold_in(jax.random.key(seed + 1), part), 4)
    hidden = jax.random.normal(part_keys[0], (2, SEQ_COUNT, SEQ_LEN, D_MODEL), jnp.float32).astype(jnp.bfloat16)
    expert_ids = jnp.stack([draw_routing(part_keys[1], 3 * MEAN_ROWS), draw_routing(part_keys[2], 2 * MEAN_ROWS)])
    gate_logits = jax.random.normal(part_keys[3], (2, SEQ_COUNT, SEQ_LEN, TOP_K), jnp.float32)
    gate_sig = jax.nn.sigmoid(gate_logits)
    gate_wts = 2.5 * gate_sig / jnp.sum(gate_sig, axis=-1, keepdims=True)
    in_scale = D_MODEL ** -0.5
    w_query = (1.2 * in_scale * jax.random.normal(shared_keys[0], (D_MODEL, N_HEADS, HEAD_DIM), jnp.float32)).astype(jnp.bfloat16)
    w_key = (1.2 * in_scale * jax.random.normal(shared_keys[1], (D_MODEL, N_HEADS, HEAD_DIM), jnp.float32)).astype(jnp.bfloat16)
    w_value = (in_scale * jax.random.normal(shared_keys[2], (D_MODEL, N_HEADS, HEAD_DIM), jnp.float32)).astype(jnp.bfloat16)
    w_out = (2.0 * PROJ_COLS ** -0.5 * jax.random.normal(shared_keys[3], (N_HEADS, HEAD_DIM, D_MODEL), jnp.float32)).astype(jnp.bfloat16)
    attn_gain = jax.random.uniform(shared_keys[4], (D_MODEL,), jnp.float32, 0.5, 1.5).astype(jnp.bfloat16)
    moe_gain = jax.random.uniform(shared_keys[5], (D_MODEL,), jnp.float32, 0.5, 1.5).astype(jnp.bfloat16)
    w_gate = (in_scale * jax.random.normal(shared_keys[6], (N_EXPERTS, D_MODEL, FF_DIM), jnp.float32)).astype(jnp.bfloat16)
    w_up = (in_scale * jax.random.normal(shared_keys[7], (N_EXPERTS, D_MODEL, FF_DIM), jnp.float32)).astype(jnp.bfloat16)
    w_down = (FF_DIM ** -0.5 * jax.random.normal(shared_keys[8], (N_EXPERTS, FF_DIM, D_MODEL), jnp.float32)).astype(jnp.bfloat16)
    return {'hidden': hidden, 'expert_ids': expert_ids, 'gate_wts': gate_wts, 'w_query': w_query, 'w_key': w_key, 'w_value': w_value, 'w_out': w_out, 'attn_gain': attn_gain, 'moe_gain': moe_gain, 'w_gate': w_gate, 'w_up': w_up, 'w_down': w_down}


def rms_norm(rows_in, gain_vec):
    rows_f32 = rows_in.astype(jnp.float32)
    inv_rms = lax.rsqrt(jnp.mean(rows_f32 * rows_f32, axis=-1, keepdims=True) + NORM_EPS)
    return (rows_f32 * inv_rms * gain_vec.astype(jnp.float32)).astype(jnp.bfloat16)


def seq_attention(seq_qkv):
    q_seq, k_seq, v_seq = seq_qkv
    scores = jnp.einsum('qhe,khe->hqk', q_seq.astype(jnp.float32), k_seq.astype(jnp.float32)) * HEAD_DIM ** -0.5
    causal = jnp.arange(SEQ_LEN)[:, None] >= jnp.arange(SEQ_LEN)[None, :]
    attn_probs = jax.nn.softmax(jnp.where(causal, scores, -jnp.inf), axis=-1).astype(jnp.bfloat16)
    attn_out = jnp.einsum('hqk,khe->qhe', attn_probs.astype(jnp.float32), v_seq.astype(jnp.float32))
    return attn_out.astype(jnp.bfloat16)


def one_expert(expert_args):
    expert_rows, gate_w, up_w, down_w = expert_args
    proj_gate = jnp.dot(expert_rows, gate_w, preferred_element_type=jnp.float32)
    proj_up = jnp.dot(expert_rows, up_w, preferred_element_type=jnp.float32)
    activated = (jax.nn.silu(proj_gate) * proj_up).astype(jnp.bfloat16)
    return jnp.dot(activated, down_w, preferred_element_type=jnp.float32).astype(jnp.bfloat16)


def micro_forward(hidden, expert_ids, gate_wts, attn_weights, moe_weights):
    w_query, w_key, w_value, w_out, attn_gain = attn_weights
    moe_gain, w_gate, w_up, w_down = moe_weights
    flat_hidden = hidden.reshape(TOKENS, D_MODEL)
    normed = rms_norm(flat_hidden, attn_gain)
    seq_shape = (SEQ_COUNT, SEQ_LEN, N_HEADS, HEAD_DIM)
    query_all = jnp.dot(normed, w_query.reshape(D_MODEL, PROJ_COLS), preferred_element_type=jnp.float32).astype(jnp.bfloat16).reshape(seq_shape)
    key_all = jnp.dot(normed, w_key.reshape(D_MODEL, PROJ_COLS), preferred_element_type=jnp.float32).astype(jnp.bfloat16).reshape(seq_shape)
    value_all = jnp.dot(normed, w_value.reshape(D_MODEL, PROJ_COLS), preferred_element_type=jnp.float32).astype(jnp.bfloat16).reshape(seq_shape)
    attn_out = lax.map(seq_attention, (query_all, key_all, value_all)).reshape(TOKENS, PROJ_COLS)
    h_mid = (flat_hidden.astype(jnp.float32) + jnp.dot(attn_out, w_out.reshape(PROJ_COLS, D_MODEL), preferred_element_type=jnp.float32)).astype(jnp.bfloat16)
    moe_in = rms_norm(h_mid, moe_gain)
    pair_total = TOKENS * TOP_K
    flat_ids = expert_ids.reshape(pair_total)
    sort_order = jnp.argsort(flat_ids, stable=True)
    counts = jnp.zeros((N_EXPERTS,), jnp.int32).at[flat_ids].add(1)
    starts = jnp.cumsum(counts) - counts
    sorted_rank = (jnp.arange(pair_total) - starts[flat_ids[sort_order]]).astype(jnp.int32)
    pair_rank = jnp.zeros((pair_total,), jnp.int32).at[sort_order].set(sorted_rank)
    token_rows = jnp.repeat(moe_in, TOP_K, axis=0)
    buffer = jnp.zeros((N_EXPERTS, EXPERT_WINDOW, D_MODEL), jnp.bfloat16).at[flat_ids, pair_rank].set(token_rows)
    expert_out = lax.map(one_expert, (buffer, w_gate, w_up, w_down))
    pair_out = expert_out[flat_ids, pair_rank].reshape(TOKENS, TOP_K, D_MODEL)
    mixed = h_mid.astype(jnp.float32) + jnp.sum(pair_out.astype(jnp.float32) * gate_wts.reshape(TOKENS, TOP_K, 1), axis=1)
    return mixed.astype(jnp.bfloat16).reshape(SEQ_COUNT, SEQ_LEN, D_MODEL)


def reference(hidden, expert_ids, gate_wts, w_query, w_key, w_value, w_out, attn_gain, moe_gain, w_gate, w_up, w_down):
    attn_weights = (w_query, w_key, w_value, w_out, attn_gain)
    moe_weights = (moe_gain, w_gate, w_up, w_down)
    micro_outs = [micro_forward(hidden[micro_idx], expert_ids[micro_idx], gate_wts[micro_idx], attn_weights, moe_weights) for micro_idx in range(2)]
    return jnp.stack(micro_outs)
```

```python
import functools

import jax
import jax.numpy as jnp
from jax import lax
from jax.experimental import pallas as pl
from jax.experimental.pallas import tpu as pltpu
from jax.sharding import PartitionSpec as P

NORM_EPS = 1e-6
EP = 128
TOK = 64
TOPK = 8
DM = 2048
HALF = DM // 2
FF = 768
CAP = 12
MAIN = 4
EXT = CAP - MAIN
GROUPS = 8
MEMB = EP // GROUPS
MESH = pl.DeviceIdType.MESH
BF = jnp.bfloat16
F32 = jnp.float32


def rms_norm(rows_in, gain_vec):
    rows_f32 = rows_in.astype(F32)
    inv_rms = lax.rsqrt(jnp.mean(rows_f32 * rows_f32, axis=-1, keepdims=True) + NORM_EPS)
    return (rows_f32 * inv_rms * gain_vec.astype(F32)).astype(BF)


def local_attention(hidden, attn_weights):
    w_query, w_key, w_value, w_out, attn_gain = attn_weights
    seq_len = hidden.shape[1]
    head_dim = w_query.shape[2]
    normed = rms_norm(hidden, attn_gain)
    query_all = jnp.einsum('btd,dhe->bthe', normed, w_query, preferred_element_type=F32).astype(BF)
    key_all = jnp.einsum('btd,dhe->bthe', normed, w_key, preferred_element_type=F32).astype(BF)
    value_all = jnp.einsum('btd,dhe->bthe', normed, w_value, preferred_element_type=F32).astype(BF)
    scores = jnp.einsum('bqhe,bkhe->bhqk', query_all, key_all, preferred_element_type=F32) * head_dim ** -0.5
    causal = jnp.arange(seq_len)[:, None] >= jnp.arange(seq_len)[None, :]
    attn_probs = jax.nn.softmax(jnp.where(causal, scores, -jnp.inf), axis=-1).astype(BF)
    attn_out = jnp.einsum('bhqk,bkhe->bqhe', attn_probs, value_all, preferred_element_type=F32).astype(BF)
    resid_sum = hidden.astype(F32) + jnp.einsum('crif,ife->cre', attn_out, w_out, preferred_element_type=F32)
    return resid_sum.astype(BF)


def split_dev(i):
    return i // 32, (i // 8) % 4, (i // 2) % 4, i % 2


def join_dev(z, y, x, c):
    return ((z * 4 + y) * 4 + x) * 2 + c


def shifted(me, d):
    mz, my, mx, mc = split_dev(me)
    dz, dy, dx, dc = split_dev(d)
    return join_dev((mz + dz) % 4, (my + dy) % 4, (mx + dx) % 4, (mc + dc) % 2)


def group_of(e):
    z, y, x, c = split_dev(e)
    return ((x + y + z) % 4) * 2 + c


def member_dev(k, i):
    z, y = i // 4, i % 4
    return join_dev(z, y, (k // 2 + 8 - y - z) % 4, k % 2)


def send_order():
    import random
    order = list(range(1, EP))
    random.Random(1).shuffle(order)
    return order


ORDER = send_order()


def greet_all(me):
    barrier = pltpu.get_barrier_semaphore()

    def body(d, carry):
        pl.semaphore_signal(barrier, inc=1, device_id={'ep': (me + d) % EP}, device_id_type=MESH)
        return carry

    lax.fori_loop(1, EP, body, 0)
    return barrier


def push(src, dst, send_sem, recv_sem, dev):
    pltpu.make_async_remote_copy(src, dst, send_sem, recv_sem, device_id={'ep': dev}, device_id_type=MESH).start()


def await_sent(ref, sem, me):
    pltpu.make_async_remote_copy(ref, ref, sem, sem, device_id={'ep': me}, device_id_type=MESH).wait_send()


def await_received(ref, sem, me):
    pltpu.make_async_remote_copy(ref, ref, sem, sem, device_id={'ep': me}, device_id_type=MESH).wait_recv()


def meta_kernel(x_ref, o_ref, send_sem, recv_sem):
    me = lax.axis_index('ep')
    barrier = greet_all(me)
    o_ref[me] = x_ref[0]
    pl.semaphore_wait(barrier, EP - 1)

    def body(d, carry):
        push(x_ref.at[0], o_ref.at[me], send_sem, recv_sem, (me + d) % EP)
        return carry

    lax.fori_loop(1, EP, body, 0)
    await_sent(o_ref.at[pl.ds(0, EP - 1)], send_sem, me)
    await_received(o_ref.at[pl.ds(0, EP - 1)], recv_sem, me)


def exchange_meta(row):
    return pl.pallas_call(
        meta_kernel,
        name='meta',
        out_shape=jax.ShapeDtypeStruct((EP, 8, 128), jnp.int32),
        in_specs=[pl.BlockSpec(memory_space=pltpu.VMEM)],
        out_specs=pl.BlockSpec(memory_space=pltpu.VMEM),
        scratch_shapes=[pltpu.SemaphoreType.DMA, pltpu.SemaphoreType.DMA],
        compiler_params=pltpu.CompilerParams(collective_id=0, has_side_effects=True),
    )(row)


def one_hot_rows(n_rows, pos_t):
    rows = lax.broadcasted_iota(jnp.int32, (n_rows, TOK), 0)
    hit = rows == pos_t[0:1, :]
    for j in range(1, TOPK):
        hit = hit | (rows == pos_t[j:j + 1, :])
    return jnp.where(hit, 1.0, 0.0).astype(BF)


def pack_into(z_ref, main_pos_ref, ext_pos_ref, main_ref, ext_ref):
    pos = main_pos_ref[...]
    step = 256
    for r in range(0, EP * 8, step):
        low = one_hot_rows(step, pos - r)
        high = one_hot_rows(step, pos + MAIN - r)
        block = jnp.dot(low, z_ref[:, :HALF], preferred_element_type=F32) + jnp.dot(high, z_ref[:, HALF:], preferred_element_type=F32)
        main_ref[r // 8:(r + step) // 8] = block.astype(BF).reshape(step // 8, 8, HALF)
    ext = jnp.dot(one_hot_rows(MEMB * EXT, ext_pos_ref[...]), z_ref[...], preferred_element_type=F32).astype(BF)
    ext_ref[...] = ext.reshape(MEMB, EXT, DM)


def dispatch_kernel(k, z_ref, main_pos_ref, ext_pos_ref, main_out, ext_out, main_buf, ext_buf, main_send, main_recv, ext_send, ext_recv, local_sem):
    me = lax.axis_index('ep')
    barrier = greet_all(me)
    pack_into(z_ref, main_pos_ref, ext_pos_ref, main_buf, ext_buf)
    pl.semaphore_wait(barrier, EP - 1)
    is_member = group_of(me) == k
    own = pltpu.make_async_copy(main_buf.at[me], main_out.at[me], local_sem.at[0])
    own.start()
    for d in ORDER:
        if d % 8 == 0:
            i = d // 8
            dest = member_dev(k, (me + i) % MEMB)

            @pl.when(dest != me)
            def _(i=i, dest=dest):
                push(ext_buf.at[(me + i) % MEMB], ext_out.at[me], ext_send, ext_recv, dest)
        dest = shifted(me, d)
        push(main_buf.at[dest], main_out.at[me], main_send, main_recv, dest)
    first = member_dev(k, me % MEMB)

    @pl.when(first != me)
    def _():
        push(ext_buf.at[me % MEMB], ext_out.at[me], ext_send, ext_recv, first)

    own.wait()
    await_sent(main_buf.at[pl.ds(0, EP - 1)], main_send, me)
    await_received(main_out.at[pl.ds(0, EP - 1)], main_recv, me)

    @pl.when(is_member)
    def _():
        mine = pltpu.make_async_copy(ext_buf.at[me // 8], ext_out.at[me], local_sem.at[1])
        mine.start()
        mine.wait()
        await_sent(ext_buf.at[pl.ds(0, MEMB - 1)], ext_send, me)
        await_received(ext_out.at[pl.ds(0, EP - 1)], ext_recv, me)

    @pl.when(jnp.logical_not(is_member))
    def _():
        await_sent(ext_buf, ext_send, me)


def dispatch(k, z, main_pos, ext_pos):
    vmem = pl.BlockSpec(memory_space=pltpu.VMEM)
    hbm = pl.BlockSpec(memory_space=pl.ANY)
    return pl.pallas_call(
        functools.partial(dispatch_kernel, k),
        name=f'dispatch{k}',
        out_shape=(jax.ShapeDtypeStruct((EP, 8, HALF), BF), jax.ShapeDtypeStruct((EP, EXT, DM), BF)),
        in_specs=[vmem] * 3,
        out_specs=(hbm, hbm),
        scratch_shapes=[
            pltpu.VMEM((EP, 8, HALF), BF),
            pltpu.VMEM((MEMB, EXT, DM), BF),
            pltpu.SemaphoreType.DMA,
            pltpu.SemaphoreType.DMA,
            pltpu.SemaphoreType.DMA,
            pltpu.SemaphoreType.DMA,
            pltpu.SemaphoreType.DMA((2,)),
        ],
        compiler_params=pltpu.CompilerParams(collective_id=1 + k, has_side_effects=True),
    )(z, main_pos, ext_pos)


def return_kernel(k, main_in, ext_in, main_out, ext_out, main_send, main_recv, ext_send, ext_recv, local_sem):
    me = lax.axis_index('ep')
    barrier = greet_all(me)
    pl.semaphore_wait(barrier, EP - 1)
    is_member = group_of(me) == k
    own = pltpu.make_async_copy(main_in.at[me], main_out.at[me], local_sem.at[0])
    own.start()

    @pl.when(is_member)
    def _():
        mine = pltpu.make_async_copy(ext_in.at[me], ext_out.at[me // 8], local_sem.at[1])
        mine.start()
        for d in ORDER:
            dest = shifted(me, d)
            push(ext_in.at[dest], ext_out.at[me // 8], ext_send, ext_recv, dest)
            push(main_in.at[dest], main_out.at[me], main_send, main_recv, dest)
        mine.wait()

    @pl.when(jnp.logical_not(is_member))
    def _():
        for d in ORDER:
            dest = shifted(me, d)
            push(main_in.at[dest], main_out.at[me], main_send, main_recv, dest)

    own.wait()
    await_sent(main_in.at[pl.ds(0, EP - 1)], main_send, me)
    await_received(main_out.at[pl.ds(0, EP - 1)], main_recv, me)

    @pl.when(is_member)
    def _():
        await_sent(ext_in.at[pl.ds(0, EP - 1)], ext_send, me)
        await_received(ext_out.at[pl.ds(0, MEMB - 1)], ext_recv, me)

    @pl.when(jnp.logical_not(is_member))
    def _():
        await_received(ext_out, ext_recv, me)


def send_back(k, main_in, ext_in):
    hbm = pl.BlockSpec(memory_space=pl.ANY)
    return pl.pallas_call(
        functools.partial(return_kernel, k),
        name=f'return{k}',
        out_shape=(jax.ShapeDtypeStruct((EP, 8, HALF), BF), jax.ShapeDtypeStruct((MEMB, EXT, DM), BF)),
        in_specs=[hbm, hbm],
        out_specs=(hbm, hbm),
        scratch_shapes=[pltpu.SemaphoreType.DMA] * 4 + [pltpu.SemaphoreType.DMA((2,))],
        compiler_params=pltpu.CompilerParams(collective_id=1 + GROUPS + k, has_side_effects=True),
    )(main_in, ext_in)


def pick_matrix(n_rows, n_cols, shift):
    row = lax.broadcasted_iota(jnp.int32, (n_rows, n_cols), 0)
    col = lax.broadcasted_iota(jnp.int32, (n_rows, n_cols), 1)
    return jnp.where(col == (row // MAIN) * 8 + row % MAIN + shift, 1.0, 0.0).astype(BF)


def place_matrix(n_rows, n_cols, shift):
    row = lax.broadcasted_iota(jnp.int32, (n_rows, n_cols), 0)
    col = lax.broadcasted_iota(jnp.int32, (n_rows, n_cols), 1)
    return jnp.where(row == (col // MAIN) * 8 + col % MAIN + shift, 1.0, 0.0).astype(BF)


def ffn_rows(rows, wg, wu, wd):
    gate = jnp.dot(rows, wg[0], preferred_element_type=F32)
    up = jnp.dot(rows, wu[0], preferred_element_type=F32)
    act = (jax.nn.silu(gate) * up).astype(BF)
    return jnp.dot(act, wd[0], preferred_element_type=F32).astype(BF)


def expert_kernel(member_ref, main_in, ext_in, wg, wu, wd, main_out, ext_out):
    pick = [pick_matrix(128, 256, 0), pick_matrix(128, 256, MAIN)]
    place = [place_matrix(256, 128, 0), place_matrix(256, 128, MAIN)]

    def main_body(b, carry):
        parts = []
        for s in range(2):
            base = pl.multiple_of(b * 64 + s * 32, 32)
            block = main_in[pl.ds(base, 32)].reshape(256, HALF)
            parts.append(jnp.concatenate([jnp.dot(m, block, preferred_element_type=F32).astype(BF) for m in pick], axis=1))
        out = ffn_rows(jnp.concatenate(parts, axis=0), wg, wu, wd)
        for s in range(2):
            base = pl.multiple_of(b * 64 + s * 32, 32)
            sub = out[s * 128:(s + 1) * 128]
            block = jnp.dot(place[0], sub[:, :HALF], preferred_element_type=F32) + jnp.dot(place[1], sub[:, HALF:], preferred_element_type=F32)
            main_out[pl.ds(base, 32)] = block.astype(BF).reshape(32, 8, HALF)
        return carry

    lax.fori_loop(0, 2, main_body, 0)

    @pl.when(member_ref[0] == 1)
    def _():
        def ext_body(b, carry):
            base = pl.multiple_of(b * 32, 32)
            rows = ext_in[pl.ds(base, 32)].reshape(256, DM)
            ext_out[pl.ds(base, 32)] = ffn_rows(rows, wg, wu, wd).reshape(32, EXT, DM)
            return carry

        lax.fori_loop(0, 4, ext_body, 0)


def run_expert(member, main_in, ext_in, w_gate, w_up, w_down):
    vmem = pl.BlockSpec(memory_space=pltpu.VMEM)
    return pl.pallas_call(
        expert_kernel,
        name='expert',
        out_shape=(jax.ShapeDtypeStruct((EP, 8, HALF), BF), jax.ShapeDtypeStruct((EP, EXT, DM), BF)),
        in_specs=[pl.BlockSpec(memory_space=pltpu.SMEM)] + [vmem] * 5,
        out_specs=(vmem, vmem),
        compiler_params=pltpu.CompilerParams(vmem_limit_bytes=56 * 1024 * 1024),
    )(member, main_in, ext_in, w_gate, w_up, w_down)


def split_weights(w):
    half = w * 0.5
    first = half.astype(BF)
    rest = half - first.astype(F32)
    second = rest.astype(BF)
    third = (rest - second.astype(F32)).astype(BF)
    return [first, second, third]


def weight_matrix(n_cols, pos, gates):
    cols = lax.broadcasted_iota(jnp.int32, (TOK, n_cols), 1)
    total = jnp.zeros((TOK, n_cols), F32)
    for j in range(TOPK):
        total = total + jnp.where(cols == pos[:, j:j + 1], gates[:, j:j + 1], 0.0)
    return total


def combine_kernel(h_ref, main_ref, ext_ref, main_pos_ref, ext_pos_ref, gate_ref, more_ref, o_ref):
    pos, gates = main_pos_ref[...], gate_ref[...]
    low = weight_matrix(EP * 8, pos, gates)
    high = weight_matrix(EP * 8, jnp.where(pos >= 0, pos + MAIN, -1), gates)
    lhs = jnp.concatenate(split_weights(low) + split_weights(high), axis=0)
    prod = jnp.dot(lhs, main_ref[...].reshape(EP * 8, HALF), preferred_element_type=F32)
    ext_lhs = jnp.concatenate(split_weights(weight_matrix(MEMB * EXT, ext_pos_ref[...], gates)), axis=0)
    ext = jnp.dot(ext_lhs, ext_ref[...].reshape(MEMB * EXT, DM), preferred_element_type=F32)

    def three(a, base):
        return a[base:base + TOK] + a[base + TOK:base + 2 * TOK] + a[base + 2 * TOK:base + 3 * TOK]

    mixed = jnp.concatenate([three(prod, 0), three(prod, 3 * TOK)], axis=1) + three(ext, 0)
    o_ref[...] = (h_ref[...].astype(F32) + (2.0 * mixed + more_ref[...])).astype(BF)


def combine(h, main, ext, main_pos, ext_pos, gates, more):
    vmem = pl.BlockSpec(memory_space=pltpu.VMEM)
    return pl.pallas_call(
        combine_kernel,
        name='combine',
        out_shape=jax.ShapeDtypeStruct((TOK, DM), BF),
        in_specs=[vmem] * 7,
        out_specs=vmem,
    )(h, main, ext, main_pos, ext_pos, gates, more)


def choice_ranks(ids):
    flat = ids.reshape(-1)
    n = flat.shape[0]
    same = flat[:, None] == flat[None, :]
    before = jnp.arange(n)[None, :] < jnp.arange(n)[:, None]
    return jnp.sum((same & before).astype(jnp.int32), axis=1).reshape(ids.shape)


def leftover_sum(z, ids, rank, left, gates, w_gate, w_up, w_down):
    slot = jnp.where(left, ids * EXT + rank - MAIN, EP * EXT).reshape(-1)
    token = jnp.full((EP * EXT,), TOK, jnp.int32).at[slot].set(jnp.arange(TOK * TOPK, dtype=jnp.int32) // TOPK, mode='drop')
    send = jnp.take(z, token, axis=0, mode='fill', fill_value=0).reshape(EP, EXT, DM)
    recv = lax.all_to_all(send, 'ep', 0, 0, tiled=True).reshape(EP * EXT, DM)
    gate = jnp.dot(recv, w_gate[0], preferred_element_type=F32)
    up = jnp.dot(recv, w_up[0], preferred_element_type=F32)
    act = (jax.nn.silu(gate) * up).astype(BF)
    out = jnp.dot(act, w_down[0], preferred_element_type=F32).astype(BF)
    back = lax.all_to_all(out.reshape(EP, EXT, DM), 'ep', 0, 0, tiled=True).reshape(EP * EXT, DM)
    rows = jnp.take(back, jnp.minimum(slot, EP * EXT - 1), axis=0).reshape(TOK, TOPK, DM)
    rows = jnp.where(left[..., None], rows.astype(F32), 0.0)
    return jnp.sum(rows * gates[..., None], axis=1)


def solution(mesh):
    tok_spec = P(None, ('dp', 'ep'))
    rep_spec = P()
    exp_spec = P('ep')

    def device_step(hidden, expert_ids, gate_wts, w_query, w_key, w_value, w_out, attn_gain, moe_gain, w_gate, w_up, w_down):
        me = lax.axis_index('ep')
        ids = [expert_ids[m, 0] for m in range(2)]
        gates = [gate_wts[m, 0] for m in range(2)]
        ranks = [choice_ranks(i) for i in ids]
        groups = [group_of(i) for i in ids]
        over = [r >= MAIN for r in ranks]
        seen = jnp.stack([jnp.any(over[m] & (groups[m] == g)) for m in range(2) for g in range(GROUPS)]).astype(jnp.int32)
        row = jnp.zeros((1, 8, 128), jnp.int32) + jnp.pad(seen, (0, 128 - 2 * GROUPS))[None, None, :]
        table = exchange_meta(row)
        union = jnp.max(table[:, 0, :2 * GROUPS], axis=0).reshape(2, GROUPS)
        chosen = [jnp.argmax(union[m]).astype(jnp.int32) for m in range(2)]
        more_needed = jnp.max(jnp.sum(union, axis=1)) > 1
        main_pos = [jnp.where(ranks[m] < MAIN, ids[m] * 8 + ranks[m], -64) for m in range(2)]
        held = [over[m] & (groups[m] == chosen[m]) for m in range(2)]
        ext_pos = [jnp.where(held[m], (ids[m] // 8) * EXT + ranks[m] - MAIN, -64) for m in range(2)]
        left = [over[m] & ~held[m] for m in range(2)]

        h_mid = local_attention(hidden[:, 0], (w_query, w_key, w_value, w_out, attn_gain))
        z = rms_norm(h_mid, moe_gain)

        more = lax.cond(
            more_needed,
            lambda: jnp.stack([leftover_sum(z[m], ids[m], ranks[m], left[m], gates[m], w_gate, w_up, w_down) for m in range(2)]),
            lambda: jnp.zeros((2, TOK, DM), F32),
        )
        outs = []
        sent = [lax.switch(chosen[m], [functools.partial(dispatch, k) for k in range(GROUPS)], z[m], main_pos[m].T, ext_pos[m].T) for m in range(2)]
        for m in range(2):
            member = (group_of(me) == chosen[m]).astype(jnp.int32).reshape(1)
            done = run_expert(member, *sent[m], w_gate, w_up, w_down)
            back = lax.switch(chosen[m], [functools.partial(send_back, k) for k in range(GROUPS)], *done)
            outs.append(combine(h_mid[m], *back, main_pos[m], ext_pos[m], gates[m], more[m]))
        return jnp.stack(outs)[:, None]

    return jax.shard_map(device_step, mesh=mesh, in_specs=(tok_spec, tok_spec, tok_spec, rep_spec, rep_spec, rep_spec, rep_spec, rep_spec, rep_spec, exp_spec, exp_spec, exp_spec), out_specs=tok_spec, check_vma=False)
```

```python
import functools

import jax
import jax.numpy as jnp
from jax import lax
from jax.experimental import pallas as pl
from jax.experimental.pallas import tpu as pltpu
from jax.sharding import PartitionSpec as P

NORM_EPS = 1e-6
EP = 128
TOK = 64
TOPK = 8
DM = 2048
HALF = DM // 2
FF = 768
CAP = 12
MAIN = 4
EXT = CAP - MAIN
GROUPS = 8
MEMB = EP // GROUPS
MESH = pl.DeviceIdType.MESH
BF = jnp.bfloat16
F32 = jnp.float32


def rms_norm(rows_in, gain_vec):
    rows_f32 = rows_in.astype(F32)
    inv_rms = lax.rsqrt(jnp.mean(rows_f32 * rows_f32, axis=-1, keepdims=True) + NORM_EPS)
    return (rows_f32 * inv_rms * gain_vec.astype(F32)).astype(BF)


def attention_rows(hidden, attn_weights):
    w_query, w_key, w_value, attn_gain = attn_weights
    seq_len = hidden.shape[1]
    head_dim = w_query.shape[2]
    normed = rms_norm(hidden, attn_gain)
    query_all = jnp.einsum('btd,dhe->bthe', normed, w_query, preferred_element_type=F32).astype(BF)
    key_all = jnp.einsum('btd,dhe->bthe', normed, w_key, preferred_element_type=F32).astype(BF)
    value_all = jnp.einsum('btd,dhe->bthe', normed, w_value, preferred_element_type=F32).astype(BF)
    scores = jnp.einsum('bqhe,bkhe->bhqk', query_all, key_all, preferred_element_type=F32) * head_dim ** -0.5
    causal = jnp.arange(seq_len)[:, None] >= jnp.arange(seq_len)[None, :]
    attn_probs = jax.nn.softmax(jnp.where(causal, scores, -jnp.inf), axis=-1).astype(BF)
    attn_out = jnp.einsum('bhqk,bkhe->bqhe', attn_probs, value_all, preferred_element_type=F32).astype(BF)
    return attn_out.reshape(-1, attn_out.shape[2] * head_dim)


def split_dev(i):
    return i // 32, (i // 8) % 4, (i // 2) % 4, i % 2


def join_dev(z, y, x, c):
    return ((z * 4 + y) * 4 + x) * 2 + c


def shifted(me, d):
    mz, my, mx, mc = split_dev(me)
    dz, dy, dx, dc = split_dev(d)
    return join_dev((mz + dz) % 4, (my + dy) % 4, (mx + dx) % 4, (mc + dc) % 2)


def group_of(e):
    z, y, x, c = split_dev(e)
    return ((x + y + z) % 4) * 2 + c


def member_dev(k, i):
    z, y = i // 4, i % 4
    return join_dev(z, y, (k // 2 + 8 - y - z) % 4, k % 2)


SKEW = (0, 7, 13, 4, 10, 1, 14, 5)


def each_peer(me, visit):
    mz, my, mx, mc = split_dev(me)

    def body(u, carry):
        for v in range(8):
            zy = (u * 5 + SKEW[v]) % 16
            dev = join_dev((mz + zy // 4) % 4, (my + zy % 4) % 4, (mx + v // 2) % 4, (mc + v % 2) % 2)
            if v == 0:

                @pl.when(zy != 0)
                def _(dev=dev):
                    visit(dev)
            else:
                visit(dev)
        return carry

    lax.fori_loop(0, 16, body, 0)


def greet_all(me):
    barrier = pltpu.get_barrier_semaphore()

    def body(d, carry):
        pl.semaphore_signal(barrier, inc=1, device_id={'ep': (me + d) % EP}, device_id_type=MESH)
        return carry

    lax.fori_loop(1, EP, body, 0)
    return barrier


def push(src, dst, send_sem, recv_sem, dev):
    pltpu.make_async_remote_copy(src, dst, send_sem, recv_sem, device_id={'ep': dev}, device_id_type=MESH).start()


def await_sent(ref, sem, me):
    pltpu.make_async_remote_copy(ref, ref, sem, sem, device_id={'ep': me}, device_id_type=MESH).wait_send()


def await_received(ref, sem, me):
    pltpu.make_async_remote_copy(ref, ref, sem, sem, device_id={'ep': me}, device_id_type=MESH).wait_recv()


VMEM = pl.BlockSpec(memory_space=pltpu.VMEM)
HBM = pl.BlockSpec(memory_space=pl.ANY)
DMA = pltpu.SemaphoreType.DMA
COMM_SEMS = [DMA, DMA, DMA, DMA, DMA((2,))]
MAIN_SHAPE = (EP, 8, HALF)
EXTRA = (8, 4)


def ext_shape(m, blocks):
    return (blocks, 8, DM if EXTRA[m] == 8 else HALF)


def comm_params(cid):
    return pltpu.CompilerParams(collective_id=cid, has_side_effects=True, vmem_limit_bytes=60 * 1024 * 1024)


OUT_STEPS = 8
OUT_SLOTS = 4


def project_kernel(att_ref, w_ref, x_ref, gain_ref, flag_ref, h_out, z_out, flags_out, w_buf, acc, w_sem, send_sem, recv_sem):
    me = lax.axis_index('ep')
    depth = w_ref.shape[0] // OUT_STEPS

    def load(i):
        rows = pl.ds(pl.multiple_of(i * depth, depth), depth)
        return pltpu.make_async_copy(w_ref.at[rows], w_buf.at[i % OUT_SLOTS], w_sem.at[i % OUT_SLOTS])

    for i in range(OUT_SLOTS - 1):
        load(i).start()
    barrier = greet_all(me)
    flags_out[me] = flag_ref[0]
    acc[...] = jnp.zeros_like(acc)

    def body(i, carry):
        @pl.when(i + OUT_SLOTS - 1 < OUT_STEPS)
        def _():
            load(i + OUT_SLOTS - 1).start()

        @pl.when(i == OUT_STEPS // 2)
        def _():
            pl.semaphore_wait(barrier, EP - 1)

            def tell(d, inner):
                push(flag_ref.at[0], flags_out.at[me], send_sem, recv_sem, (me + d) % EP)
                return inner

            lax.fori_loop(1, EP, tell, 0)

        load(i).wait()
        cols = pl.ds(pl.multiple_of(i * depth, depth), depth)
        acc[...] += jnp.dot(att_ref[:, cols], w_buf[i % OUT_SLOTS], preferred_element_type=F32)
        return carry

    lax.fori_loop(0, OUT_STEPS, body, 0)
    h_mid = (x_ref[...].astype(F32) + acc[...]).astype(BF)
    h_out[...] = h_mid
    z_out[...] = rms_norm(h_mid, gain_ref[...])
    await_sent(flags_out.at[pl.ds(0, EP - 1)], send_sem, me)
    await_received(flags_out.at[pl.ds(0, EP - 1)], recv_sem, me)


def project(att, w_out, x, gain, flags):
    rows = x.shape[0]
    depth = w_out.shape[0] // OUT_STEPS
    return pl.pallas_call(
        project_kernel,
        name='project',
        out_shape=(jax.ShapeDtypeStruct(x.shape, BF), jax.ShapeDtypeStruct(x.shape, BF), jax.ShapeDtypeStruct((EP, 8, 128), jnp.int32)),
        in_specs=[VMEM, HBM, VMEM, VMEM, VMEM],
        out_specs=(VMEM, VMEM, VMEM),
        scratch_shapes=[
            pltpu.VMEM((OUT_SLOTS, depth, DM), BF),
            pltpu.VMEM((rows, DM), F32),
            DMA((OUT_SLOTS,)),
            DMA,
            DMA,
        ],
        compiler_params=comm_params(0),
    )(att, w_out, x, gain, flags)


def one_hot_rows(n_rows, pos_t, base):
    rows = lax.broadcasted_iota(jnp.int32, (n_rows, TOK), 0) + base
    hit = rows == pos_t[0:1, :]
    for j in range(1, TOPK):
        hit = hit | (rows == pos_t[j:j + 1, :])
    return jnp.where(hit, 1.0, 0.0).astype(BF)


def pack_halves(z_ref, pos, base, n_rows):
    low = one_hot_rows(n_rows, pos, base)
    high = one_hot_rows(n_rows, pos + MAIN, base)
    block = jnp.dot(low, z_ref[:, :HALF], preferred_element_type=F32) + jnp.dot(high, z_ref[:, HALF:], preferred_element_type=F32)
    return block.astype(BF).reshape(n_rows // 8, 8, HALF)


def pack_into(m, z_ref, main_pos_ref, ext_pos_ref, main_v, ext_v, main_hbm, ext_hbm, sem):
    pos = main_pos_ref[...]
    step = 256

    def body(r, carry):
        main_v[pl.ds(pl.multiple_of(r * (step // 8), step // 8), step // 8)] = pack_halves(z_ref, pos, r * step, step)
        return carry

    if EXTRA[m] == 8:
        ext = jnp.dot(one_hot_rows(MEMB * 8, ext_pos_ref[...], 0), z_ref[...], preferred_element_type=F32).astype(BF)
        ext_v[...] = ext.reshape(MEMB, 8, DM)
    else:
        ext_v[...] = pack_halves(z_ref, ext_pos_ref[...], 0, MEMB * 8)
    ext_copy = pltpu.make_async_copy(ext_v, ext_hbm, sem.at[1])
    ext_copy.start()
    lax.fori_loop(0, EP * 8 // step, body, 0)
    main_copy = pltpu.make_async_copy(main_v, main_hbm, sem.at[0])
    main_copy.start()
    ext_copy.wait()
    main_copy.wait()


def dispatch_start(k, me, main_buf, ext_buf, main_out, ext_out, main_send, main_recv, ext_send, ext_recv, local_sem):
    pltpu.make_async_copy(main_buf.at[me], main_out.at[me], local_sem.at[0]).start()

    def extra(j, carry):
        i = (me + j * 5) % MEMB
        dest = member_dev(k, i)

        @pl.when(dest != me)
        def _():
            push(ext_buf.at[i], ext_out.at[me], ext_send, ext_recv, dest)

        @pl.when(dest == me)
        def _():
            pltpu.make_async_copy(ext_buf.at[i], ext_out.at[me], local_sem.at[1]).start()

        return carry

    lax.fori_loop(0, MEMB, extra, 0)
    each_peer(me, lambda dev: push(main_buf.at[dev], main_out.at[me], main_send, main_recv, dev))


def dispatch_wait(k, me, main_buf, ext_buf, main_out, ext_out, main_send, main_recv, ext_send, ext_recv, local_sem):
    is_member = group_of(me) == k
    pltpu.make_async_copy(main_buf.at[me], main_out.at[me], local_sem.at[0]).wait()
    await_sent(main_buf.at[pl.ds(0, EP - 1)], main_send, me)
    await_received(main_out.at[pl.ds(0, EP - 1)], main_recv, me)

    @pl.when(is_member)
    def _():
        pltpu.make_async_copy(ext_buf.at[me // 8], ext_out.at[me], local_sem.at[1]).wait()
        await_sent(ext_buf.at[pl.ds(0, MEMB - 1)], ext_send, me)
        await_received(ext_out.at[pl.ds(0, EP - 1)], ext_recv, me)

    @pl.when(jnp.logical_not(is_member))
    def _():
        await_sent(ext_buf, ext_send, me)


def return_start(k, me, main_in, ext_in, main_out, ext_out, main_send, main_recv, ext_send, ext_recv, local_sem):
    is_member = group_of(me) == k
    pltpu.make_async_copy(main_in.at[me], main_out.at[me], local_sem.at[0]).start()

    @pl.when(is_member)
    def _():
        pltpu.make_async_copy(ext_in.at[me], ext_out.at[me // 8], local_sem.at[1]).start()
        each_peer(me, lambda dev: push(ext_in.at[dev], ext_out.at[me // 8], ext_send, ext_recv, dev))

    each_peer(me, lambda dev: push(main_in.at[dev], main_out.at[me], main_send, main_recv, dev))


def return_wait(k, me, main_in, ext_in, main_out, ext_out, main_send, main_recv, ext_send, ext_recv, local_sem):
    is_member = group_of(me) == k
    pltpu.make_async_copy(main_in.at[me], main_out.at[me], local_sem.at[0]).wait()
    await_sent(main_in.at[pl.ds(0, EP - 1)], main_send, me)
    await_received(main_out.at[pl.ds(0, EP - 1)], main_recv, me)

    @pl.when(is_member)
    def _():
        pltpu.make_async_copy(ext_in.at[me], ext_out.at[me // 8], local_sem.at[1]).wait()
        await_sent(ext_in.at[pl.ds(0, EP - 1)], ext_send, me)
        await_received(ext_out.at[pl.ds(0, MEMB - 1)], ext_recv, me)

    @pl.when(jnp.logical_not(is_member))
    def _():
        await_received(ext_out, ext_recv, me)


def pick_matrix(n_rows, n_cols, shift):
    row = lax.broadcasted_iota(jnp.int32, (n_rows, n_cols), 0)
    col = lax.broadcasted_iota(jnp.int32, (n_rows, n_cols), 1)
    return jnp.where(col == (row // MAIN) * 8 + row % MAIN + shift, 1.0, 0.0).astype(BF)


def place_matrix(n_rows, n_cols, shift):
    row = lax.broadcasted_iota(jnp.int32, (n_rows, n_cols), 0)
    col = lax.broadcasted_iota(jnp.int32, (n_rows, n_cols), 1)
    return jnp.where(row == (col // MAIN) * 8 + col % MAIN + shift, 1.0, 0.0).astype(BF)


def expert_scratch(m):
    blocks = EP // 2 + (EP if EXTRA[m] == 8 else EP // 2)
    return [
        pltpu.VMEM((EP if EXTRA[m] == 8 else 2 * EP, 8, HALF), BF),
        pltpu.VMEM((blocks, 8, DM), BF),
        pltpu.VMEM((blocks, 8, DM), BF),
        pltpu.VMEM((256, FF), BF),
        pltpu.VMEM((DM, FF), BF),
        pltpu.VMEM((DM, FF), BF),
        pltpu.VMEM((FF, DM), BF),
        DMA((7,)),
    ]


def expert_copies(m, refs, scratch):
    main_in, ext_in, wg, wu, wd, main_out, ext_out = refs
    main_v, rows_v, outs_v, _, wg_v, wu_v, wd_v, sem = scratch
    if EXTRA[m] == 8:
        ext_from, ext_to = outs_v.at[pl.ds(EP // 2, EP)], rows_v.at[pl.ds(EP // 2, EP)]
    else:
        ext_from = ext_to = main_v.at[pl.ds(EP, EP)]
    main_part = main_v.at[pl.ds(0, EP)]
    pairs = [(main_in, main_part), (ext_in, ext_to), (wg.at[0], wg_v), (wu.at[0], wu_v), (wd.at[0], wd_v)]
    loads = [pltpu.make_async_copy(a, b, sem.at[i]) for i, (a, b) in enumerate(pairs)]
    stores = [
        pltpu.make_async_copy(main_part, main_out, sem.at[5]),
        pltpu.make_async_copy(ext_from, ext_out, sem.at[6]),
    ]
    return loads, stores


def expert_load(m, refs, scratch):
    for copy in expert_copies(m, refs, scratch)[0]:
        copy.start()


def expert_compute(m, refs, scratch):
    loads, stores = expert_copies(m, refs, scratch)
    main_v, rows_v, outs_v, act_v, wg_v, wu_v, wd_v, _ = scratch
    halves = main_v.shape[0] // 32
    loads[0].wait()
    loads[1].wait()

    def unpack(b, carry):
        block = main_v[pl.ds(pl.multiple_of(b * 32, 32), 32)].reshape(256, HALF)
        for part in range(2):
            picked = jnp.dot(pick_matrix(128, 256, part * MAIN), block, preferred_element_type=F32).astype(BF)
            rows_v[pl.ds(pl.multiple_of(b * 16, 16), 16), :, part * HALF:(part + 1) * HALF] = picked.reshape(16, 8, HALF)
        return carry

    lax.fori_loop(0, halves, unpack, 0)
    for copy in loads[2:]:
        copy.wait()

    def ffn(b, carry):
        base = pl.multiple_of(b * 32, 32)
        rows = rows_v[pl.ds(base, 32)].reshape(256, DM)

        def hidden(n, inner):
            cols = pl.ds(pl.multiple_of(n * 256, 256), 256)
            gate = jnp.dot(rows, wg_v[:, cols], preferred_element_type=F32)
            up = jnp.dot(rows, wu_v[:, cols], preferred_element_type=F32)
            act_v[:, cols] = (jax.nn.silu(gate) * up).astype(BF)
            return inner

        lax.fori_loop(0, FF // 256, hidden, 0)

        def down(n, inner):
            cols = pl.ds(pl.multiple_of(n * 512, 512), 512)
            out = jnp.dot(act_v[...], wd_v[:, cols], preferred_element_type=F32).astype(BF)
            outs_v[pl.ds(base, 32), :, cols] = out.reshape(32, 8, 512)
            return inner

        lax.fori_loop(0, DM // 512, down, 0)
        return carry

    lax.fori_loop(0, rows_v.shape[0] // 32, ffn, 0)

    def place(b, carry):
        sub = outs_v[pl.ds(pl.multiple_of(b * 16, 16), 16)].reshape(128, DM)
        block = jnp.dot(place_matrix(256, 128, 0), sub[:, :HALF], preferred_element_type=F32)
        block = block + jnp.dot(place_matrix(256, 128, MAIN), sub[:, HALF:], preferred_element_type=F32)
        main_v[pl.ds(pl.multiple_of(b * 32, 32), 32)] = block.astype(BF).reshape(32, 8, HALF)
        return carry

    lax.fori_loop(0, halves, place, 0)
    for copy in stores:
        copy.start()
    for copy in stores:
        copy.wait()


def split_weights(w):
    half = w * 0.5
    first = half.astype(BF)
    rest = half - first.astype(F32)
    second = rest.astype(BF)
    third = (rest - second.astype(F32)).astype(BF)
    return [first, second, third]


def weight_matrix(n_cols, pos, gates):
    cols = lax.broadcasted_iota(jnp.int32, (TOK, n_cols), 1)
    total = jnp.zeros((TOK, n_cols), F32)
    for j in range(TOPK):
        total = total + jnp.where(cols == pos[:, j:j + 1], gates[:, j:j + 1], 0.0)
    return total


LHS_SHAPE = (6 * TOK, EP * 8)
CHUNK = 256


def combine_rows(m, h_ref, main_ref, ext_ref, main_pos_ref, ext_pos_ref, gate_ref, more_ref, o_ref, lhs_ref):
    gates, pos, ext_pos = gate_ref[m], main_pos_ref[m], ext_pos_ref[m]

    def stack(n_cols, at):
        return jnp.concatenate(split_weights(weight_matrix(n_cols, at, gates)) + split_weights(weight_matrix(n_cols, at + MAIN, gates)), axis=0)

    def weights(c, carry):
        base = pl.multiple_of(c * CHUNK, CHUNK)
        lhs_ref[:, pl.ds(base, CHUNK)] = stack(CHUNK, pos - base)
        return carry

    lax.fori_loop(0, EP * 8 // CHUNK, weights, 0)
    if EXTRA[m] == 8:
        ext_lhs = jnp.concatenate(split_weights(weight_matrix(MEMB * 8, ext_pos, gates)), axis=0)
    else:
        ext_lhs = stack(MEMB * 8, ext_pos)

    def three(a):
        return a[:TOK] + a[TOK:2 * TOK] + a[2 * TOK:]

    def columns(c, carry):
        base = pl.multiple_of(c * CHUNK, CHUNK)
        prod = jnp.dot(lhs_ref[...], main_ref[:, :, pl.ds(base, CHUNK)].reshape(EP * 8, CHUNK), preferred_element_type=F32)
        if EXTRA[m] == 4:
            both = jnp.dot(ext_lhs, ext_ref[:, :, pl.ds(base, CHUNK)].reshape(MEMB * 8, CHUNK), preferred_element_type=F32)
        for part in range(2):
            cols = pl.ds(pl.multiple_of(part * HALF + base, CHUNK), CHUNK)
            if EXTRA[m] == 4:
                ext = both[part * 3 * TOK:(part + 1) * 3 * TOK]
            else:
                ext = jnp.dot(ext_lhs, ext_ref[:, :, cols].reshape(MEMB * 8, CHUNK), preferred_element_type=F32)
            mixed = three(prod[part * 3 * TOK:(part + 1) * 3 * TOK]) + three(ext)
            o_ref[m, :, cols] = (h_ref[m, :, cols].astype(F32) + (2.0 * mixed + more_ref[m, :, cols])).astype(BF)
        return carry

    lax.fori_loop(0, HALF // CHUNK, columns, 0)


def sds(shape):
    return jax.ShapeDtypeStruct(shape, BF)


def pack_scratch(m):
    return [pltpu.VMEM(MAIN_SHAPE, BF), pltpu.VMEM(ext_shape(m, MEMB), BF), DMA((2,))]


def dispatch_kernel(k, m, with_expert, *args):
    me = lax.axis_index('ep')
    z_ref, main_pos_ref, ext_pos_ref = args[:3]
    args = args[3:]
    if with_expert:
        expert_in, args = args[:5], args[5:]
    main_out, ext_out, main_stage, ext_stage = args[:4]
    args = args[4:]
    if with_expert:
        expert_out, args = args[:2], args[2:]
    main_v, ext_v, pack_sem = args[:3]
    sems, scratch = args[3:8], args[8:]
    barrier = greet_all(me)
    if with_expert:
        refs = tuple(expert_in) + tuple(expert_out)
        expert_load(1 - m, refs, scratch)
    pack_into(m, z_ref, main_pos_ref, ext_pos_ref, main_v, ext_v, main_stage, ext_stage, pack_sem)
    pl.semaphore_wait(barrier, EP - 1)
    dispatch_start(k, me, main_stage, ext_stage, main_out, ext_out, *sems)
    if with_expert:
        expert_compute(1 - m, refs, scratch)
    dispatch_wait(k, me, main_stage, ext_stage, main_out, ext_out, *sems)


def dispatch(k, z, main_pos, ext_pos):
    m = 0
    outs = pl.pallas_call(
        functools.partial(dispatch_kernel, k, m, False),
        name=f'dispatch{k}',
        out_shape=(sds(MAIN_SHAPE), sds(ext_shape(m, EP)), sds(MAIN_SHAPE), sds(ext_shape(m, MEMB))),
        in_specs=[VMEM] * 3,
        out_specs=(HBM,) * 4,
        scratch_shapes=pack_scratch(m) + COMM_SEMS,
        compiler_params=comm_params(1 + k),
    )(z, main_pos, ext_pos)
    return outs[:2]


def dispatch_expert(k, z, main_pos, ext_pos, main_in, ext_in, w_gate, w_up, w_down):
    m = 1
    outs = pl.pallas_call(
        functools.partial(dispatch_kernel, k, m, True),
        name=f'dispatch_expert{k}',
        out_shape=(sds(MAIN_SHAPE), sds(ext_shape(m, EP)), sds(MAIN_SHAPE), sds(ext_shape(m, MEMB)), sds(MAIN_SHAPE), sds(ext_shape(1 - m, EP))),
        in_specs=[VMEM] * 3 + [HBM] * 5,
        out_specs=(HBM,) * 6,
        scratch_shapes=pack_scratch(m) + COMM_SEMS + expert_scratch(1 - m),
        compiler_params=comm_params(1 + GROUPS + k),
    )(z, main_pos, ext_pos, main_in, ext_in, w_gate, w_up, w_down)
    return outs[0], outs[1], outs[4], outs[5]


def return_expert_kernel(k, main_ret, ext_ret, main_in, ext_in, wg, wu, wd, main_out, ext_out, main_done, ext_done, *rest):
    me = lax.axis_index('ep')
    sems, scratch = rest[:5], rest[5:]
    refs = (main_in, ext_in, wg, wu, wd, main_done, ext_done)
    barrier = greet_all(me)
    expert_load(1, refs, scratch)
    pl.semaphore_wait(barrier, EP - 1)
    return_start(k, me, main_ret, ext_ret, main_out, ext_out, *sems)
    expert_compute(1, refs, scratch)
    return_wait(k, me, main_ret, ext_ret, main_out, ext_out, *sems)


def return_expert(k, main_ret, ext_ret, main_in, ext_in, w_gate, w_up, w_down):
    return pl.pallas_call(
        functools.partial(return_expert_kernel, k),
        name=f'return_expert{k}',
        out_shape=(sds(MAIN_SHAPE), sds(ext_shape(0, MEMB)), sds(MAIN_SHAPE), sds(ext_shape(1, EP))),
        in_specs=[HBM] * 7,
        out_specs=(HBM,) * 4,
        scratch_shapes=COMM_SEMS + expert_scratch(1),
        compiler_params=comm_params(1 + 2 * GROUPS + k),
    )(main_ret, ext_ret, main_in, ext_in, w_gate, w_up, w_down)


def return_combine_kernel(k, main_ret, ext_ret, main_a, ext_a, h_ref, main_pos_ref, ext_pos_ref, gate_ref, more_ref, o_ref, main_buf, ext_buf, lhs_ref, *sems):
    me = lax.axis_index('ep')
    barrier = greet_all(me)
    pl.semaphore_wait(barrier, EP - 1)
    return_start(k, me, main_ret, ext_ret, main_buf, ext_buf, *sems)
    shared = (main_pos_ref, ext_pos_ref, gate_ref, more_ref, o_ref, lhs_ref)
    combine_rows(0, h_ref, main_a, ext_a, *shared)
    return_wait(k, me, main_ret, ext_ret, main_buf, ext_buf, *sems)
    combine_rows(1, h_ref, main_buf, ext_buf, *shared)


def return_combine(k, main_ret, ext_ret, main_a, ext_a, h, main_pos, ext_pos, gates, more):
    return pl.pallas_call(
        functools.partial(return_combine_kernel, k),
        name=f'return_combine{k}',
        out_shape=sds((2, TOK, DM)),
        in_specs=[HBM] * 2 + [VMEM] * 7,
        out_specs=VMEM,
        scratch_shapes=[pltpu.VMEM(MAIN_SHAPE, BF), pltpu.VMEM(ext_shape(1, MEMB), BF), pltpu.VMEM(LHS_SHAPE, BF)] + COMM_SEMS,
        compiler_params=comm_params(1 + 3 * GROUPS + k),
    )(main_ret, ext_ret, main_a, ext_a, h, main_pos, ext_pos, gates, more)


def choice_ranks(ids):
    flat = ids.reshape(2, -1)
    n = flat.shape[1]
    same = flat[:, :, None] == flat[:, None, :]
    before = jnp.arange(n)[None, :] < jnp.arange(n)[:, None]
    return jnp.sum((same & before).astype(jnp.int32), axis=2).reshape(ids.shape)


def leftover_rows_kernel(rows_ref, wg, wu, wd, o_ref):
    def hidden(n):
        cols = pl.ds(pl.multiple_of(n * 256, 256), 256)
        gate = jnp.dot(rows_ref[...], wg[0, :, cols], preferred_element_type=F32)
        up = jnp.dot(rows_ref[...], wu[0, :, cols], preferred_element_type=F32)
        act = (jax.nn.silu(gate) * up).astype(BF)
        return jnp.dot(act, wd[0, cols, :], preferred_element_type=F32)

    o_ref[...] = lax.fori_loop(0, FF // 256, lambda n, acc: acc + hidden(n), jnp.zeros(o_ref.shape, F32)).astype(BF)


def leftover_rows(rows, w_gate, w_up, w_down):
    spec = pl.BlockSpec((128, DM), lambda i: (i, 0))
    return pl.pallas_call(
        leftover_rows_kernel,
        name='leftover',
        out_shape=sds(rows.shape),
        grid=(rows.shape[0] // 128,),
        in_specs=[spec, VMEM, VMEM, VMEM],
        out_specs=spec,
    )(rows, w_gate, w_up, w_down)


def leftover_sum(z, ids, rank, left, gates, weights):
    slot = jnp.where(left, ids * EXT + rank - MAIN, EP * EXT).reshape(-1)
    token = jnp.full((EP * EXT,), TOK, jnp.int32).at[slot].set(jnp.arange(TOK * TOPK, dtype=jnp.int32) // TOPK, mode='drop')
    send = jnp.take(z, token, axis=0, mode='fill', fill_value=0).reshape(EP, EXT, DM)
    recv = lax.all_to_all(send, 'ep', 0, 0, tiled=True).reshape(EP * EXT, DM)
    out = leftover_rows(recv, *weights)
    back = lax.all_to_all(out.reshape(EP, EXT, DM), 'ep', 0, 0, tiled=True).reshape(EP * EXT, DM)
    rows = jnp.take(back, jnp.minimum(slot, EP * EXT - 1), axis=0).reshape(TOK, TOPK, DM)
    rows = jnp.where(left[..., None], rows.astype(F32), 0.0)
    return jnp.sum(rows * gates[..., None], axis=1)


def solution(mesh):
    tok_spec = P(None, ('dp', 'ep'))
    rep_spec = P()
    exp_spec = P('ep')

    def device_step(hidden, expert_ids, gate_wts, w_query, w_key, w_value, w_out, attn_gain, moe_gain, w_gate, w_up, w_down):
        ids, gates = expert_ids[:, 0], gate_wts[:, 0]
        ranks = choice_ranks(ids)
        groups = group_of(ids)
        over = ranks >= MAIN
        lanes = jnp.arange(128, dtype=jnp.int32)
        marks = [jnp.any(over[m][..., None] & (groups[m][..., None] + m * GROUPS == lanes), axis=(0, 1)) for m in range(2)]
        beyond = jnp.any(ranks[1] >= MAIN + EXTRA[1]) & (lanes == 2 * GROUPS)
        flags = jnp.broadcast_to((marks[0] | marks[1] | beyond).astype(jnp.int32), (1, 8, 128))

        att = attention_rows(hidden[:, 0], (w_query, w_key, w_value, attn_gain))
        h_mid, z, table = project(att, w_out.reshape(-1, DM), hidden.reshape(2 * TOK, DM), moe_gain.reshape(1, DM), flags)
        h_mid, z = h_mid.reshape(2, TOK, DM), z.reshape(2, TOK, DM)

        union = jnp.max(table[:, 0, :2 * GROUPS], axis=0).reshape(2, GROUPS)
        chosen = jnp.argmax(union, axis=1).astype(jnp.int32)
        more_needed = (jnp.max(jnp.sum(union, axis=1)) > 1) | jnp.any(table[:, 0, 2 * GROUPS] > 0)
        extra = jnp.array(EXTRA, jnp.int32)[:, None, None]
        held = over & (groups == chosen[:, None, None]) & (ranks < MAIN + extra)
        left = over & ~held
        main_pos = jnp.where(over, -4096, ids * 8 + ranks)
        ext_pos = jnp.where(held, (ids // 8) * 8 + ranks - MAIN, -4096)
        main_pos_t, ext_pos_t = main_pos.transpose(0, 2, 1), ext_pos.transpose(0, 2, 1)

        more = lax.cond(
            more_needed,
            lambda: lax.map(lambda a: leftover_sum(*a, (w_gate, w_up, w_down)), (z, ids, ranks, left, gates)),
            lambda: jnp.zeros((2, TOK, DM), F32),
        )

        def choose(m, fn, *args):
            return lax.switch(chosen[m], [functools.partial(fn, k) for k in range(GROUPS)], *args)

        weights = (w_gate, w_up, w_down)
        sent_a = choose(0, dispatch, z[0], main_pos_t[0], ext_pos_t[0])
        main_b, ext_b, *done_a = choose(1, dispatch_expert, z[1], main_pos_t[1], ext_pos_t[1], *sent_a, *weights)
        main_a, ext_a, *done_b = choose(0, return_expert, *done_a, main_b, ext_b, *weights)
        mixed = choose(1, return_combine, *done_b, main_a, ext_a, h_mid, main_pos, ext_pos, gates, more)
        return mixed[:, None]

    return jax.shard_map(device_step, mesh=mesh, in_specs=(tok_spec, tok_spec, tok_spec, rep_spec, rep_spec, rep_spec, rep_spec, rep_spec, rep_spec, exp_spec, exp_spec, exp_spec), out_specs=tok_spec, check_vma=False)
```

```python
import functools

import jax
import jax.numpy as jnp
from jax import lax
from jax.experimental import pallas as pl
from jax.experimental.pallas import tpu as pltpu
from jax.sharding import PartitionSpec as P

NORM_EPS = 1e-6
EP = 128
TOK = 64
TOPK = 8
DM = 2048
HALF = DM // 2
FF = 768
CAP = 12
MAIN = 4
EXT = CAP - MAIN
GROUPS = 8
MEMB = EP // GROUPS
MESH = pl.DeviceIdType.MESH
BF = jnp.bfloat16
F32 = jnp.float32


def rms_norm(rows_in, gain_vec):
    rows_f32 = rows_in.astype(F32)
    inv_rms = lax.rsqrt(jnp.mean(rows_f32 * rows_f32, axis=-1, keepdims=True) + NORM_EPS)
    return (rows_f32 * inv_rms * gain_vec.astype(F32)).astype(BF)


def attention_rows(hidden, attn_weights):
    w_query, w_key, w_value, attn_gain = attn_weights
    seq_len = hidden.shape[1]
    head_dim = w_query.shape[2]
    normed = rms_norm(hidden, attn_gain)
    query_all = jnp.einsum('btd,dhe->bthe', normed, w_query, preferred_element_type=F32).astype(BF)
    key_all = jnp.einsum('btd,dhe->bthe', normed, w_key, preferred_element_type=F32).astype(BF)
    value_all = jnp.einsum('btd,dhe->bthe', normed, w_value, preferred_element_type=F32).astype(BF)
    scores = jnp.einsum('bqhe,bkhe->bhqk', query_all, key_all, preferred_element_type=F32) * head_dim ** -0.5
    causal = jnp.arange(seq_len)[:, None] >= jnp.arange(seq_len)[None, :]
    attn_probs = jax.nn.softmax(jnp.where(causal, scores, -jnp.inf), axis=-1).astype(BF)
    attn_out = jnp.einsum('bhqk,bkhe->bqhe', attn_probs, value_all, preferred_element_type=F32).astype(BF)
    return attn_out.reshape(-1, attn_out.shape[2] * head_dim)


def split_dev(i):
    return i // 32, (i // 8) % 4, (i // 2) % 4, i % 2


def join_dev(z, y, x, c):
    return ((z * 4 + y) * 4 + x) * 2 + c


def shifted(me, d):
    mz, my, mx, mc = split_dev(me)
    dz, dy, dx, dc = split_dev(d)
    return join_dev((mz + dz) % 4, (my + dy) % 4, (mx + dx) % 4, (mc + dc) % 2)


def group_of(e):
    z, y, x, c = split_dev(e)
    return ((x + y + z) % 4) * 2 + c


def member_dev(k, i):
    z, y = i // 4, i % 4
    return join_dev(z, y, (k // 2 + 8 - y - z) % 4, k % 2)


def each_peer(me, visit):
    mz, my, mx, mc = split_dev(me)

    def body(s, carry):
        u, v = s // 8, s % 8
        zy = (u * 5 + v * 7) % 16
        dev = join_dev((mz + zy // 4) % 4, (my + zy % 4) % 4, (mx + v // 2) % 4, (mc + v % 2) % 2)
        visit(dev)
        return carry

    lax.fori_loop(1, EP, body, 0)


def greet_all(me):
    barrier = pltpu.get_barrier_semaphore()

    def body(d, carry):
        pl.semaphore_signal(barrier, inc=1, device_id={'ep': (me + d) % EP}, device_id_type=MESH)
        return carry

    lax.fori_loop(1, EP, body, 0)
    return barrier


def push(src, dst, send_sem, recv_sem, dev):
    pltpu.make_async_remote_copy(src, dst, send_sem, recv_sem, device_id={'ep': dev}, device_id_type=MESH).start()


def await_sent(ref, sem, me):
    pltpu.make_async_remote_copy(ref, ref, sem, sem, device_id={'ep': me}, device_id_type=MESH).wait_send()


def await_received(ref, sem, me):
    pltpu.make_async_remote_copy(ref, ref, sem, sem, device_id={'ep': me}, device_id_type=MESH).wait_recv()


VMEM = pl.BlockSpec(memory_space=pltpu.VMEM)
HBM = pl.BlockSpec(memory_space=pl.ANY)
DMA = pltpu.SemaphoreType.DMA
COMM_SEMS = [DMA, DMA, DMA, DMA, DMA((2,))]
MAIN_SHAPE = (EP, 8, HALF)
EXTRA = (8, 4)
GROUP_CODE = 1024
NOWHERE = -65536


def ext_shape(m, blocks):
    return (blocks, 8, DM if EXTRA[m] == 8 else HALF)


def comm_params(cid):
    return pltpu.CompilerParams(collective_id=cid, has_side_effects=True, vmem_limit_bytes=60 * 1024 * 1024)


OUT_STEPS = 8
OUT_SLOTS = 4


def project_kernel(att_ref, w_ref, x_ref, gain_ref, flag_ref, h_out, z_out, union_out, w_buf, acc, flags_out, w_sem, send_sem, recv_sem):
    me = lax.axis_index('ep')
    depth = w_ref.shape[0] // OUT_STEPS

    def load(i):
        rows = pl.ds(pl.multiple_of(i * depth, depth), depth)
        return pltpu.make_async_copy(w_ref.at[rows], w_buf.at[i % OUT_SLOTS], w_sem.at[i % OUT_SLOTS])

    for i in range(OUT_SLOTS - 1):
        load(i).start()
    flags_out[me] = flag_ref[0]
    barrier = greet_all(me)
    acc[...] = jnp.zeros_like(acc)

    def body(i, carry):
        @pl.when(i + OUT_SLOTS - 1 < OUT_STEPS)
        def _():
            load(i + OUT_SLOTS - 1).start()

        @pl.when(i == OUT_STEPS // 2)
        def _():
            pl.semaphore_wait(barrier, EP - 1)

            def tell(d, inner):
                push(flag_ref.at[0], flags_out.at[me], send_sem, recv_sem, (me + d) % EP)
                return inner

            lax.fori_loop(1, EP, tell, 0)

        load(i).wait()
        cols = pl.ds(pl.multiple_of(i * depth, depth), depth)
        acc[...] += jnp.dot(att_ref[:, cols], w_buf[i % OUT_SLOTS], preferred_element_type=F32)
        return carry

    lax.fori_loop(0, OUT_STEPS, body, 0)
    h_mid = (x_ref[...].astype(F32) + acc[...]).astype(BF)
    h_out[...] = h_mid
    z_out[...] = rms_norm(h_mid, gain_ref[...])
    await_sent(flags_out.at[pl.ds(0, EP - 1)], send_sem, me)
    await_received(flags_out.at[pl.ds(0, EP - 1)], recv_sem, me)
    union_out[...] = jnp.max(flags_out[...], axis=0)


def project(att, w_out, x, gain, flags):
    rows = x.shape[0]
    depth = w_out.shape[0] // OUT_STEPS
    return pl.pallas_call(
        project_kernel,
        name='project',
        out_shape=(jax.ShapeDtypeStruct(x.shape, BF), jax.ShapeDtypeStruct(x.shape, BF), jax.ShapeDtypeStruct((8, 128), jnp.int32)),
        in_specs=[VMEM, HBM, VMEM, VMEM, VMEM],
        out_specs=(VMEM, VMEM, VMEM),
        scratch_shapes=[
            pltpu.VMEM((OUT_SLOTS, depth, DM), BF),
            pltpu.VMEM((rows, DM), F32),
            pltpu.VMEM((EP, 8, 128), jnp.int32),
            DMA((OUT_SLOTS,)),
            DMA,
            DMA,
        ],
        compiler_params=comm_params(0),
    )(att, w_out, x, gain, flags)


def one_hot_rows(n_rows, pos_t, base):
    rows = lax.broadcasted_iota(jnp.int32, (n_rows, TOK), 0) + base
    hit = rows == pos_t[0:1, :]
    for j in range(1, TOPK):
        hit = hit | (rows == pos_t[j:j + 1, :])
    return jnp.where(hit, 1.0, 0.0).astype(BF)


def pack_halves(m, z_ref, pos, base, n_rows):
    low = one_hot_rows(n_rows, pos, base)
    high = one_hot_rows(n_rows, pos + MAIN, base)
    block = jnp.dot(low, z_ref[m, :, :HALF], preferred_element_type=F32) + jnp.dot(high, z_ref[m, :, HALF:], preferred_element_type=F32)
    return block.astype(BF).reshape(n_rows // 8, 8, HALF)


def pack_into(k, m, z_ref, main_pos_ref, ext_pos_ref, main_v, ext_v, main_hbm, ext_hbm, sem):
    pos = main_pos_ref[m]
    ext_pos = ext_pos_ref[m] - k * GROUP_CODE
    step = 256

    def body(r, carry):
        main_v[pl.ds(pl.multiple_of(r * (step // 8), step // 8), step // 8)] = pack_halves(m, z_ref, pos, r * step, step)
        return carry

    if EXTRA[m] == 8:
        ext = jnp.dot(one_hot_rows(MEMB * 8, ext_pos, 0), z_ref[m], preferred_element_type=F32).astype(BF)
        ext_v[...] = ext.reshape(MEMB, 8, DM)
    else:
        ext_v[...] = pack_halves(m, z_ref, ext_pos, 0, MEMB * 8)
    ext_copy = pltpu.make_async_copy(ext_v, ext_hbm, sem.at[1])
    ext_copy.start()
    lax.fori_loop(0, EP * 8 // step, body, 0)
    main_copy = pltpu.make_async_copy(main_v, main_hbm, sem.at[0])
    main_copy.start()
    ext_copy.wait()
    main_copy.wait()


def dispatch_start(k, me, main_buf, ext_buf, main_out, ext_out, main_send, main_recv, ext_send, ext_recv, local_sem):
    pltpu.make_async_copy(main_buf.at[me], main_out.at[me], local_sem.at[0]).start()

    def extra(j, carry):
        i = (me + j * 5) % MEMB
        dest = member_dev(k, i)

        @pl.when(dest != me)
        def _():
            push(ext_buf.at[i], ext_out.at[me], ext_send, ext_recv, dest)

        @pl.when(dest == me)
        def _():
            pltpu.make_async_copy(ext_buf.at[i], ext_out.at[me], local_sem.at[1]).start()

        return carry

    lax.fori_loop(0, MEMB, extra, 0)
    each_peer(me, lambda dev: push(main_buf.at[dev], main_out.at[me], main_send, main_recv, dev))


def dispatch_wait(k, me, main_buf, ext_buf, main_out, ext_out, main_send, main_recv, ext_send, ext_recv, local_sem):
    is_member = group_of(me) == k
    pltpu.make_async_copy(main_buf.at[me], main_out.at[me], local_sem.at[0]).wait()
    await_sent(main_buf.at[pl.ds(0, EP - 1)], main_send, me)
    await_received(main_out.at[pl.ds(0, EP - 1)], main_recv, me)

    @pl.when(is_member)
    def _():
        pltpu.make_async_copy(ext_buf.at[me // 8], ext_out.at[me], local_sem.at[1]).wait()
        await_sent(ext_buf.at[pl.ds(0, MEMB - 1)], ext_send, me)
        await_received(ext_out.at[pl.ds(0, EP - 1)], ext_recv, me)

    @pl.when(jnp.logical_not(is_member))
    def _():
        await_sent(ext_buf, ext_send, me)


def return_start(k, me, main_in, ext_in, main_out, ext_out, main_send, main_recv, ext_send, ext_recv, local_sem):
    is_member = group_of(me) == k
    pltpu.make_async_copy(main_in.at[me], main_out.at[me], local_sem.at[0]).start()

    @pl.when(is_member)
    def _():
        pltpu.make_async_copy(ext_in.at[me], ext_out.at[me // 8], local_sem.at[1]).start()
        each_peer(me, lambda dev: push(ext_in.at[dev], ext_out.at[me // 8], ext_send, ext_recv, dev))

    each_peer(me, lambda dev: push(main_in.at[dev], main_out.at[me], main_send, main_recv, dev))


def return_wait(k, me, main_in, ext_in, main_out, ext_out, main_send, main_recv, ext_send, ext_recv, local_sem):
    is_member = group_of(me) == k
    pltpu.make_async_copy(main_in.at[me], main_out.at[me], local_sem.at[0]).wait()
    await_sent(main_in.at[pl.ds(0, EP - 1)], main_send, me)
    await_received(main_out.at[pl.ds(0, EP - 1)], main_recv, me)

    @pl.when(is_member)
    def _():
        pltpu.make_async_copy(ext_in.at[me], ext_out.at[me // 8], local_sem.at[1]).wait()
        await_sent(ext_in.at[pl.ds(0, EP - 1)], ext_send, me)
        await_received(ext_out.at[pl.ds(0, MEMB - 1)], ext_recv, me)

    @pl.when(jnp.logical_not(is_member))
    def _():
        await_received(ext_out, ext_recv, me)


def pick_matrix(n_rows, n_cols, shift):
    row = lax.broadcasted_iota(jnp.int32, (n_rows, n_cols), 0)
    col = lax.broadcasted_iota(jnp.int32, (n_rows, n_cols), 1)
    return jnp.where(col == (row // MAIN) * 8 + row % MAIN + shift, 1.0, 0.0).astype(BF)


def place_matrix(n_rows, n_cols, shift):
    row = lax.broadcasted_iota(jnp.int32, (n_rows, n_cols), 0)
    col = lax.broadcasted_iota(jnp.int32, (n_rows, n_cols), 1)
    return jnp.where(row == (col // MAIN) * 8 + col % MAIN + shift, 1.0, 0.0).astype(BF)


ROWS = (256, 128)


def expert_scratch(m):
    blocks = EP // 2 + (EP if EXTRA[m] == 8 else EP // 2)
    return [
        pltpu.VMEM((EP if EXTRA[m] == 8 else 2 * EP, 8, HALF), BF),
        pltpu.VMEM((blocks, 8, DM), BF),
        pltpu.VMEM((blocks, 8, DM), BF),
        pltpu.VMEM((ROWS[m], FF), BF),
        pltpu.VMEM((DM, FF), BF),
        pltpu.VMEM((DM, FF), BF),
        pltpu.VMEM((FF, DM), BF),
        DMA((7,)),
    ]


def expert_copies(m, refs, scratch):
    main_in, ext_in, wg, wu, wd, main_out, ext_out = refs
    main_v, rows_v, outs_v, _, wg_v, wu_v, wd_v, sem = scratch
    if EXTRA[m] == 8:
        ext_from, ext_to = outs_v.at[pl.ds(EP // 2, EP)], rows_v.at[pl.ds(EP // 2, EP)]
    else:
        ext_from = ext_to = main_v.at[pl.ds(EP, EP)]
    main_part = main_v.at[pl.ds(0, EP)]
    pairs = [(main_in, main_part), (ext_in, ext_to), (wg.at[0], wg_v), (wu.at[0], wu_v), (wd.at[0], wd_v)]
    loads = [pltpu.make_async_copy(a, b, sem.at[i]) for i, (a, b) in enumerate(pairs)]
    stores = [
        pltpu.make_async_copy(main_part, main_out, sem.at[5]),
        pltpu.make_async_copy(ext_from, ext_out, sem.at[6]),
    ]
    return loads, stores


def expert_load(m, refs, scratch):
    for copy in expert_copies(m, refs, scratch)[0]:
        copy.start()


def expert_compute(m, refs, scratch):
    loads, stores = expert_copies(m, refs, scratch)
    main_v, rows_v, outs_v, act_v, wg_v, wu_v, wd_v, _ = scratch
    halves, n_rows = main_v.shape[0] // 32, ROWS[m]
    loads[0].wait()
    loads[1].wait()

    def unpack(b, carry):
        block = main_v[pl.ds(pl.multiple_of(b * 32, 32), 32)].reshape(256, HALF)
        for part in range(2):
            picked = jnp.dot(pick_matrix(128, 256, part * MAIN), block, preferred_element_type=F32).astype(BF)
            rows_v[pl.ds(pl.multiple_of(b * 16, 16), 16), :, part * HALF:(part + 1) * HALF] = picked.reshape(16, 8, HALF)
        return carry

    lax.fori_loop(0, halves, unpack, 0)
    for copy in loads[2:]:
        copy.wait()

    def ffn(b, carry):
        base = pl.multiple_of(b * (n_rows // 8), n_rows // 8)
        rows = rows_v[pl.ds(base, n_rows // 8)].reshape(n_rows, DM)

        def hidden(n, inner):
            cols = pl.ds(pl.multiple_of(n * 256, 256), 256)
            gate = jnp.dot(rows, wg_v[:, cols], preferred_element_type=F32)
            up = jnp.dot(rows, wu_v[:, cols], preferred_element_type=F32)
            act_v[:, cols] = (jax.nn.silu(gate) * up).astype(BF)
            return inner

        lax.fori_loop(0, FF // 256, hidden, 0)

        def down(n, inner):
            cols = pl.ds(pl.multiple_of(n * 512, 512), 512)
            out = jnp.dot(act_v[...], wd_v[:, cols], preferred_element_type=F32).astype(BF)
            outs_v[pl.ds(base, n_rows // 8), :, cols] = out.reshape(n_rows // 8, 8, 512)
            return inner

        lax.fori_loop(0, DM // 512, down, 0)
        return carry

    lax.fori_loop(0, rows_v.shape[0] * 8 // n_rows, ffn, 0)

    def place(b, carry):
        sub = outs_v[pl.ds(pl.multiple_of(b * 16, 16), 16)].reshape(128, DM)
        block = jnp.dot(place_matrix(256, 128, 0), sub[:, :HALF], preferred_element_type=F32)
        block = block + jnp.dot(place_matrix(256, 128, MAIN), sub[:, HALF:], preferred_element_type=F32)
        main_v[pl.ds(pl.multiple_of(b * 32, 32), 32)] = block.astype(BF).reshape(32, 8, HALF)
        return carry

    lax.fori_loop(0, halves, place, 0)
    for copy in stores:
        copy.start()
    for copy in stores:
        copy.wait()


def split_weights(w):
    half = w * 0.5
    first = half.astype(BF)
    rest = half - first.astype(F32)
    second = rest.astype(BF)
    third = (rest - second.astype(F32)).astype(BF)
    return [first, second, third]


def weight_matrix(n_cols, pos, gates):
    cols = lax.broadcasted_iota(jnp.int32, (TOK, n_cols), 1)
    total = jnp.zeros((TOK, n_cols), F32)
    for j in range(TOPK):
        total = total + jnp.where(cols == pos[:, j:j + 1], gates[:, j:j + 1], 0.0)
    return total


LHS_SHAPE = (6 * TOK, EP * 8)
CHUNK = 256


def combine_rows(m, h_ref, main_ref, ext_ref, main_pos_ref, ext_pos_ref, gate_ref, more_ref, o_ref, lhs_ref):
    gates, pos, ext_pos = gate_ref[m], main_pos_ref[m], ext_pos_ref[m]

    def stack(n_cols, at):
        return jnp.concatenate(split_weights(weight_matrix(n_cols, at, gates)) + split_weights(weight_matrix(n_cols, at + MAIN, gates)), axis=0)

    def weights(c, carry):
        base = pl.multiple_of(c * CHUNK, CHUNK)
        lhs_ref[:, pl.ds(base, CHUNK)] = stack(CHUNK, pos - base)
        return carry

    lax.fori_loop(0, EP * 8 // CHUNK, weights, 0)
    if EXTRA[m] == 8:
        ext_lhs = jnp.concatenate(split_weights(weight_matrix(MEMB * 8, ext_pos, gates)), axis=0)
    else:
        ext_lhs = stack(MEMB * 8, ext_pos)

    def three(a):
        return a[:TOK] + a[TOK:2 * TOK] + a[2 * TOK:]

    def columns(c, carry):
        base = pl.multiple_of(c * CHUNK, CHUNK)
        prod = jnp.dot(lhs_ref[...], main_ref[:, :, pl.ds(base, CHUNK)].reshape(EP * 8, CHUNK), preferred_element_type=F32)
        if EXTRA[m] == 4:
            both = jnp.dot(ext_lhs, ext_ref[:, :, pl.ds(base, CHUNK)].reshape(MEMB * 8, CHUNK), preferred_element_type=F32)
        for part in range(2):
            cols = pl.ds(pl.multiple_of(part * HALF + base, CHUNK), CHUNK)
            if EXTRA[m] == 4:
                ext = both[part * 3 * TOK:(part + 1) * 3 * TOK]
            else:
                ext = jnp.dot(ext_lhs, ext_ref[:, :, cols].reshape(MEMB * 8, CHUNK), preferred_element_type=F32)
            mixed = three(prod[part * 3 * TOK:(part + 1) * 3 * TOK]) + three(ext)
            o_ref[m, :, cols] = (h_ref[m, :, cols].astype(F32) + (2.0 * mixed + more_ref[m, :, cols])).astype(BF)
        return carry

    lax.fori_loop(0, HALF // CHUNK, columns, 0)


def sds(shape):
    return jax.ShapeDtypeStruct(shape, BF)


def pack_scratch(m):
    return [pltpu.VMEM(MAIN_SHAPE, BF), pltpu.VMEM(ext_shape(m, MEMB), BF), DMA((2,))]


def dispatch_kernel(k, m, with_expert, *args):
    me = lax.axis_index('ep')
    z_ref, main_pos_ref, ext_pos_ref = args[:3]
    args = args[3:]
    if with_expert:
        expert_in, args = args[:5], args[5:]
    main_out, ext_out, main_stage, ext_stage = args[:4]
    args = args[4:]
    if with_expert:
        expert_out, args = args[:2], args[2:]
    main_v, ext_v, pack_sem = args[:3]
    sems, scratch = args[3:8], args[8:]
    barrier = greet_all(me)
    if with_expert:
        refs = tuple(expert_in) + tuple(expert_out)
        expert_load(1 - m, refs, scratch)
    pack_into(k, m, z_ref, main_pos_ref, ext_pos_ref, main_v, ext_v, main_stage, ext_stage, pack_sem)
    pl.semaphore_wait(barrier, EP - 1)
    dispatch_start(k, me, main_stage, ext_stage, main_out, ext_out, *sems)
    if with_expert:
        expert_compute(1 - m, refs, scratch)
    dispatch_wait(k, me, main_stage, ext_stage, main_out, ext_out, *sems)


def dispatch(k, z, main_pos, ext_pos):
    m = 0
    outs = pl.pallas_call(
        functools.partial(dispatch_kernel, k, m, False),
        name=f'dispatch{k}',
        out_shape=(sds(MAIN_SHAPE), sds(ext_shape(m, EP)), sds(MAIN_SHAPE), sds(ext_shape(m, MEMB))),
        in_specs=[VMEM] * 3,
        out_specs=(HBM,) * 4,
        scratch_shapes=pack_scratch(m) + COMM_SEMS,
        compiler_params=comm_params(1 + k),
    )(z, main_pos, ext_pos)
    return outs[:2]


def dispatch_expert(k, z, main_pos, ext_pos, main_in, ext_in, w_gate, w_up, w_down):
    m = 1
    outs = pl.pallas_call(
        functools.partial(dispatch_kernel, k, m, True),
        name=f'dispatch_expert{k}',
        out_shape=(sds(MAIN_SHAPE), sds(ext_shape(m, EP)), sds(MAIN_SHAPE), sds(ext_shape(m, MEMB)), sds(MAIN_SHAPE), sds(ext_shape(1 - m, EP))),
        in_specs=[VMEM] * 3 + [HBM] * 5,
        out_specs=(HBM,) * 6,
        scratch_shapes=pack_scratch(m) + COMM_SEMS + expert_scratch(1 - m),
        compiler_params=comm_params(1 + GROUPS + k),
    )(z, main_pos, ext_pos, main_in, ext_in, w_gate, w_up, w_down)
    return outs[0], outs[1], outs[4], outs[5]


def return_expert_kernel(k, main_ret, ext_ret, main_in, ext_in, wg, wu, wd, main_out, ext_out, main_done, ext_done, *rest):
    me = lax.axis_index('ep')
    sems, scratch = rest[:5], rest[5:]
    refs = (main_in, ext_in, wg, wu, wd, main_done, ext_done)
    barrier = greet_all(me)
    expert_load(1, refs, scratch)
    pl.semaphore_wait(barrier, EP - 1)
    return_start(k, me, main_ret, ext_ret, main_out, ext_out, *sems)
    expert_compute(1, refs, scratch)
    return_wait(k, me, main_ret, ext_ret, main_out, ext_out, *sems)


def return_expert(k, main_ret, ext_ret, main_in, ext_in, w_gate, w_up, w_down):
    return pl.pallas_call(
        functools.partial(return_expert_kernel, k),
        name=f'return_expert{k}',
        out_shape=(sds(MAIN_SHAPE), sds(ext_shape(0, MEMB)), sds(MAIN_SHAPE), sds(ext_shape(1, EP))),
        in_specs=[HBM] * 7,
        out_specs=(HBM,) * 4,
        scratch_shapes=COMM_SEMS + expert_scratch(1),
        compiler_params=comm_params(1 + 2 * GROUPS + k),
    )(main_ret, ext_ret, main_in, ext_in, w_gate, w_up, w_down)


def return_combine_kernel(k, main_ret, ext_ret, main_a, ext_a, h_ref, main_pos_ref, ext_pos_ref, gate_ref, more_ref, o_ref, main_buf, ext_buf, lhs_ref, *sems):
    me = lax.axis_index('ep')
    barrier = greet_all(me)
    pl.semaphore_wait(barrier, EP - 1)
    return_start(k, me, main_ret, ext_ret, main_buf, ext_buf, *sems)
    shared = (main_pos_ref, ext_pos_ref, gate_ref, more_ref, o_ref, lhs_ref)
    combine_rows(0, h_ref, main_a, ext_a, *shared)
    return_wait(k, me, main_ret, ext_ret, main_buf, ext_buf, *sems)
    combine_rows(1, h_ref, main_buf, ext_buf, *shared)


def return_combine(k, main_ret, ext_ret, main_a, ext_a, h, main_pos, ext_pos, gates, more):
    return pl.pallas_call(
        functools.partial(return_combine_kernel, k),
        name=f'return_combine{k}',
        out_shape=sds((2, TOK, DM)),
        in_specs=[HBM] * 2 + [VMEM] * 7,
        out_specs=VMEM,
        scratch_shapes=[pltpu.VMEM(MAIN_SHAPE, BF), pltpu.VMEM(ext_shape(1, MEMB), BF), pltpu.VMEM(LHS_SHAPE, BF)] + COMM_SEMS,
        compiler_params=comm_params(1 + 3 * GROUPS + k),
    )(main_ret, ext_ret, main_a, ext_a, h, main_pos, ext_pos, gates, more)


def choice_ranks(ids):
    flat = ids.reshape(2, -1)
    n = flat.shape[1]
    same = flat[:, :, None] == flat[:, None, :]
    before = jnp.arange(n)[None, :] < jnp.arange(n)[:, None]
    return jnp.sum((same & before).astype(jnp.int32), axis=2).reshape(ids.shape)


def leftover_rows_kernel(rows_ref, wg, wu, wd, o_ref):
    def hidden(n):
        cols = pl.ds(pl.multiple_of(n * 256, 256), 256)
        gate = jnp.dot(rows_ref[...], wg[0, :, cols], preferred_element_type=F32)
        up = jnp.dot(rows_ref[...], wu[0, :, cols], preferred_element_type=F32)
        act = (jax.nn.silu(gate) * up).astype(BF)
        return jnp.dot(act, wd[0, cols, :], preferred_element_type=F32)

    o_ref[...] = lax.fori_loop(0, FF // 256, lambda n, acc: acc + hidden(n), jnp.zeros(o_ref.shape, F32)).astype(BF)


def leftover_rows(rows, w_gate, w_up, w_down):
    spec = pl.BlockSpec((128, DM), lambda i: (i, 0))
    return pl.pallas_call(
        leftover_rows_kernel,
        name='leftover',
        out_shape=sds(rows.shape),
        grid=(rows.shape[0] // 128,),
        in_specs=[spec, VMEM, VMEM, VMEM],
        out_specs=spec,
    )(rows, w_gate, w_up, w_down)


def leftover_sum(z, ids, rank, left, gates, weights):
    slot = jnp.where(left, ids * EXT + rank - MAIN, EP * EXT).reshape(-1)
    token = jnp.full((EP * EXT,), TOK, jnp.int32).at[slot].set(jnp.arange(TOK * TOPK, dtype=jnp.int32) // TOPK, mode='drop')
    send = jnp.take(z, token, axis=0, mode='fill', fill_value=0).reshape(EP, EXT, DM)
    recv = lax.all_to_all(send, 'ep', 0, 0, tiled=True).reshape(EP * EXT, DM)
    out = leftover_rows(recv, *weights)
    back = lax.all_to_all(out.reshape(EP, EXT, DM), 'ep', 0, 0, tiled=True).reshape(EP * EXT, DM)
    rows = jnp.take(back, jnp.minimum(slot, EP * EXT - 1), axis=0).reshape(TOK, TOPK, DM)
    rows = jnp.where(left[..., None], rows.astype(F32), 0.0)
    return jnp.sum(rows * gates[..., None], axis=1)


def solution(mesh):
    tok_spec = P(None, ('dp', 'ep'))
    rep_spec = P()
    exp_spec = P('ep')

    def device_step(hidden, expert_ids, gate_wts, w_query, w_key, w_value, w_out, attn_gain, moe_gain, w_gate, w_up, w_down):
        ids, gates = expert_ids[:, 0], gate_wts[:, 0]
        ranks = choice_ranks(ids)
        groups = group_of(ids)
        over = ranks >= MAIN
        lanes = jnp.arange(128, dtype=jnp.int32)
        marks = [jnp.any(over[m][..., None] & (groups[m][..., None] + m * GROUPS == lanes), axis=(0, 1)) for m in range(2)]
        beyond = jnp.any(ranks[1] >= MAIN + EXTRA[1]) & (lanes == 2 * GROUPS)
        flags = jnp.broadcast_to((marks[0] | marks[1] | beyond).astype(jnp.int32), (1, 8, 128))

        main_pos = jnp.where(over, NOWHERE, ids * 8 + ranks)
        extra = jnp.array(EXTRA, jnp.int32)[:, None, None]
        ext_code = jnp.where(over & (ranks < MAIN + extra), groups * GROUP_CODE + (ids // 8) * 8 + ranks - MAIN, NOWHERE)
        main_pos_t, ext_code_t = main_pos.transpose(0, 2, 1), ext_code.transpose(0, 2, 1)

        att = attention_rows(hidden[:, 0], (w_query, w_key, w_value, attn_gain))
        h_mid, z, table = project(att, w_out.reshape(-1, DM), hidden.reshape(2 * TOK, DM), moe_gain.reshape(1, DM), flags)
        h_mid, z = h_mid.reshape(2, TOK, DM), z.reshape(2, TOK, DM)

        union = table[0, :2 * GROUPS].reshape(2, GROUPS)
        chosen = jnp.argmax(union, axis=1).astype(jnp.int32)
        more_needed = (jnp.max(jnp.sum(union, axis=1)) > 1) | (table[0, 2 * GROUPS] > 0)
        ext_pos = ext_code - chosen[:, None, None] * GROUP_CODE

        def leftovers():
            held = (ext_pos >= 0) & (ext_pos < GROUP_CODE)
            return lax.map(lambda a: leftover_sum(*a, (w_gate, w_up, w_down)), (z, ids, ranks, over & ~held, gates))

        more = lax.cond(more_needed, leftovers, lambda: jnp.zeros((2, TOK, DM), F32))

        def choose(m, fn, *args):
            return lax.switch(chosen[m], [functools.partial(fn, k) for k in range(GROUPS)], *args)

        weights = (w_gate, w_up, w_down)
        sent_a = choose(0, dispatch, z, main_pos_t, ext_code_t)
        main_b, ext_b, *done_a = choose(1, dispatch_expert, z, main_pos_t, ext_code_t, *sent_a, *weights)
        main_a, ext_a, *done_b = choose(0, return_expert, *done_a, main_b, ext_b, *weights)
        mixed = choose(1, return_combine, *done_b, main_a, ext_a, h_mid, main_pos, ext_pos, gates, more)
        return mixed[:, None]

    return jax.shard_map(device_step, mesh=mesh, in_specs=(tok_spec, tok_spec, tok_spec, rep_spec, rep_spec, rep_spec, rep_spec, rep_spec, rep_spec, exp_spec, exp_spec, exp_spec), out_specs=tok_spec, check_vma=False)
```
